32 devices in a mesh: dp: 16 (over z, x, core), tensor: 2 (over y).
Axes of the slice: x: 2, y: 2, z: 4, core: 2. Of those that a mesh axis runs over, the one named last changes fastest.
Arguments:
- residual: bfloat16 [4096, 4096], P('dp', 'tensor'), may hold values from -6 to 6
- fresh_qkv: bfloat16 [4096, 3, 2048], P('dp', None, 'tensor'), may hold values from -110 to 110
- active: int32 [4096], P('dp'), may hold values from 0 to 1
- home_slot: int32 [4096], P('dp'), may hold values from 0 to 4095, as said below
- kv_cache: bfloat16 [4096, 2, 16, 2048], P('dp', None, None, 'tensor'), may hold values from -6 to 6
- lengths: int32 [4096], P('dp'), may hold values from 2 to 16
- w_out: bfloat16 [2048, 4096], P('tensor'), may hold values from -0.125 to 0.125
Outputs:
- updated: bfloat16 [4096, 4096], P('dp', 'tensor')
The draws below stay inside these ranges and needn't reach their ends.
Inputs may be any that keep to these rules, and one draw needn't show every extreme that they name: Each dp group owns the slots 256 * g to 256 * g + 255; home_slot is a permutation. Among the streams of one dp group, at most 16 active streams have slots in the same owning group, and this is reached in every draw.
All inputs are finite; a program needn't handle non-finite values.
Results may differ from the reference program's by a relative error of at most 0.0062.
Values may be sent and summed in bfloat16 or wider, within the bound.
No kernel may reach another device: no remote copies, remote signals or barrier semaphores. Data moves between devices by JAX's collectives and lax.ppermute only.
A program may use at most 128 MiB of HBM per device.

```python
import jax
import jax.numpy as jnp
from jax import lax

D = 4096
HEADS = 16
HD = 128
S_DEV = 256
L = 16
CAP = 16
STREAMS = 4096


def routing(key):
    base = jax.random.fold_in(key, 101)
    groups = STREAMS // S_DEV
    stream_index = jnp.arange(STREAMS, dtype=jnp.int32)
    source = stream_index // S_DEV
    within = stream_index % S_DEV
    shuffled = jax.random.permutation(jax.random.fold_in(base, 1), groups).astype(jnp.int32)
    inverse = jnp.argsort(shuffled).astype(jnp.int32)
    values = jnp.arange(groups, dtype=jnp.int32)
    priority = jnp.where(values == 1, 0, jnp.where(values == groups - 1, 1, jnp.where(values == groups // 2, 2, 3 + inverse)))
    offsets = jnp.argsort(priority).astype(jnp.int32)[:S_DEV // CAP]
    owner_group = (source + offsets[within // CAP]) % groups
    ranking = jax.random.randint(jax.random.fold_in(base, 2), (groups, S_DEV), 0, 1 << 20) * S_DEV + jnp.arange(S_DEV, dtype=jnp.int32)[None, :]
    slot_order = jnp.argsort(ranking, axis=1).astype(jnp.int32)
    home_slot = owner_group * S_DEV + slot_order[owner_group, within]
    active_level = jax.random.randint(jax.random.fold_in(base, 3), (groups,), 2, 9)
    dice_roll = jax.random.randint(jax.random.fold_in(base, 4), (STREAMS,), 0, 8)
    active = jnp.logical_or(dice_roll < active_level[owner_group], stream_index < CAP)
    return (home_slot.astype(jnp.int32), active.astype(jnp.int32))


def draw_home_slot(key, part):
    return routing(key)[0]


def draw_active(key, part):
    return routing(key)[1]


def draw_fresh_qkv(key, part):
    drawn = jnp.clip(jax.random.normal(jax.random.fold_in(key, 201), (STREAMS, 3, HEADS * HD), jnp.float32), -6.0, 6.0)
    return drawn.astype(jnp.bfloat16)


def draw_kv_cache(key, part):
    drawn = jnp.clip(jax.random.normal(jax.random.fold_in(key, 202), (STREAMS, 2, L, HEADS * HD), jnp.float32), -6.0, 6.0)
    return drawn.astype(jnp.bfloat16)


def place_ends(array, stream_key, least, top_value):
    longest = array.shape.index(max(array.shape))
    spots = []
    for shift in (0, 1):
        where = [jax.random.randint(jax.random.fold_in(stream_key, axis), (), 0, length) for axis, length in enumerate(array.shape)]
        where[longest] = (where[longest] + shift) % array.shape[longest]
        spots.append(tuple(where))
    return array.at[spots[0]].set(least).at[spots[1]].set(top_value)


def level_of(own_key, shape, shards, least, largest):
    factor_of = 1.0
    for position, shards_of in shards:
        draws = jax.random.uniform(jax.random.fold_in(jax.random.fold_in(own_key, 6), position), (shards_of,), jnp.float32, least / len(shards), largest / len(shards))
        factor_of = factor_of * jnp.repeat(jnp.exp(draws), shape[position] // shards_of).reshape((-1,) + (1,) * (len(shape) - 1 - position))
    return factor_of


def bell_draw(own_key, extent, width, most, split=(), held_as=jnp.bfloat16):
    result = jax.random.normal(own_key, extent, jnp.float32) * width
    if len(split) > 0:
        result = level_of(own_key, extent, split, -0.22, 0.18) * result
    return jnp.clip(result, min=-most, max=most).astype(held_as)


def setup_inputs(seed: int = 0) -> dict:
    keys = jax.random.split(jax.random.key(seed), 8)
    return {
        "residual": bell_draw(keys[0], (STREAMS, D), 1.0, 6.0, ((0, 16), (1, 2))),
        "fresh_qkv": draw_fresh_qkv(jax.random.fold_in(keys[7], 71), 0),
        "active": draw_active(jax.random.fold_in(keys[7], 71), 0),
        "home_slot": draw_home_slot(jax.random.fold_in(keys[7], 71), 0),
        "kv_cache": draw_kv_cache(jax.random.fold_in(keys[7], 71), 0),
        "lengths": place_ends(jax.random.randint(keys[5], (STREAMS,), 2, L + 1), jax.random.fold_in(keys[5], 1), 2, L).astype(jnp.int32),
        "w_out": bell_draw(keys[6], (HEADS * HD, D), (HEADS * HD) ** -0.5, 0.125, ((0, 2),)),
    }


def attend(query, key_rows, value_rows, key_new, value_new, length):
    score_scale = HD ** -0.5
    scores = jnp.einsum("bhd,blhd->bhl", query.astype(jnp.float32), key_rows.astype(jnp.float32)) * score_scale
    positions = jnp.arange(L, dtype=jnp.int32)
    in_cache = positions[None, None, :] < length[:, None, None]
    scores = jnp.where(in_cache, scores, jnp.float32(-1e30))
    own_score = jnp.sum(query.astype(jnp.float32) * key_new.astype(jnp.float32), axis=-1) * score_scale
    row_max = jnp.maximum(jnp.max(scores, axis=-1), own_score)
    weights_raw = jnp.exp(scores - row_max[..., None])
    own_raw = jnp.exp(own_score - row_max)
    denominator = jnp.sum(weights_raw, axis=-1) + own_raw
    weights = (weights_raw / denominator[..., None]).astype(jnp.bfloat16)
    own_weight = (own_raw / denominator).astype(jnp.bfloat16)
    mixed = jnp.einsum("bhl,blhd->bhd", weights.astype(jnp.float32), value_rows.astype(jnp.float32))
    mixed = mixed + own_weight.astype(jnp.float32)[..., None] * value_new.astype(jnp.float32)
    return mixed.astype(jnp.bfloat16).reshape(query.shape[0], -1)


def reference(residual, fresh_qkv, active, home_slot, kv_cache, lengths, w_out):
    groups = STREAMS // S_DEV

    def one_group(group):
        start = (group * S_DEV).astype(jnp.int32)
        streams = start + jnp.arange(S_DEV, dtype=jnp.int32)
        slots = home_slot[streams]
        fresh_rows = jnp.take(fresh_qkv, streams, axis=0).reshape(S_DEV, 3, HEADS, HD)
        cache_rows = jnp.take(kv_cache, slots, axis=0).reshape(S_DEV, 2, L, HEADS, HD)
        attended = attend(fresh_rows[:, 0], cache_rows[:, 0], cache_rows[:, 1], fresh_rows[:, 1], fresh_rows[:, 2], lengths[slots])
        projected = jnp.dot(attended, w_out, preferred_element_type=jnp.float32)
        rows = lax.dynamic_slice_in_dim(residual, start, S_DEV, 0).astype(jnp.float32)
        flags = active[streams].astype(jnp.float32)
        return (rows + flags[:, None] * projected).astype(jnp.bfloat16)

    updated = lax.map(one_group, jnp.arange(groups, dtype=jnp.int32))
    return updated.reshape(STREAMS, D)
```

```python
import functools

import jax
import jax.numpy as jnp
from jax import lax
from jax.experimental import pallas as pl
from jax.experimental.pallas import tpu as pltpu
from jax.sharding import PartitionSpec as P

HD = 128
LANES = 128
ID_BASE = 128
F32 = jnp.float32
BF16 = jnp.bfloat16


def vmem():
    return pl.BlockSpec(memory_space=pltpu.VMEM)


def dot(a, b, dims=((1,), (0,))):
    return lax.dot_general(a, b, (dims, ((), ())), preferred_element_type=F32)


def cost(flops, bytes_accessed):
    return pl.CostEstimate(flops=flops, bytes_accessed=bytes_accessed, transcendentals=0)


def route_kernel(streams, capacity, home_ref, active_ref, query_ref, send_ref, placing_ref):
    rows = send_ref.shape[0]
    width = query_ref.shape[1]
    home = home_ref[...]
    is_active = active_ref[...] > 0
    owner = home // streams
    code_row = jnp.where(is_active, owner, -1).astype(F32)
    code_col = jnp.transpose(jnp.broadcast_to(code_row, (streams, streams)))
    before = lax.broadcasted_iota(jnp.int32, (streams, streams), 0) < lax.broadcasted_iota(
        jnp.int32, (streams, streams), 1
    )
    rank = jnp.sum(
        jnp.where((code_col == code_row) & before, 1.0, 0.0), axis=0, keepdims=True
    ).astype(jnp.int32)
    target = jnp.where(is_active, owner * capacity + rank, -1)
    placing = jnp.where(
        lax.broadcasted_iota(jnp.int32, (rows, streams), 0) == target, 1.0, 0.0
    ).astype(BF16)
    placing_ref[...] = placing
    send_ref[:, :width] = dot(placing, query_ref[...]).astype(BF16)
    local = home - owner * streams
    kind = lax.broadcasted_iota(jnp.int32, (LANES, streams), 0)
    ids = jnp.where(
        kind == 0, local // ID_BASE, jnp.where(kind == 1, local % ID_BASE, jnp.where(kind == 2, 1, 0))
    )
    send_ref[:, width:] = dot(placing, ids.astype(F32).astype(BF16), ((1,), (1,))).astype(BF16)


def route(home, active, query, capacity, groups):
    streams, width = query.shape
    rows = groups * capacity
    return pl.pallas_call(
        functools.partial(route_kernel, streams, capacity),
        out_shape=(
            jax.ShapeDtypeStruct((rows, width + LANES), BF16),
            jax.ShapeDtypeStruct((rows, streams), BF16),
        ),
        in_specs=[vmem()] * 3,
        out_specs=(vmem(), vmem()),
        cost_estimate=cost(2 * rows * streams * (width + LANES), 4 * streams * width),
        name="route",
    )(home.reshape(1, streams), active.reshape(1, streams), query)


def attend_kernel(heads, block, pair, got_ref, bias_ref, kv_ref, back_ref, owned_ref, mixed_ref):
    step = pl.program_id(0)
    rows, padded = got_ref.shape
    slots = owned_ref.shape[0]
    cache_len = kv_ref.shape[2]
    width = heads * HD
    scale = HD ** (-0.5)

    def matched():
        tail = got_ref[:, width:].astype(F32)
        local = (tail[:, 0:1] * ID_BASE + tail[:, 1:2]).astype(jnp.int32)
        local = jnp.where(tail[:, 2:3] > 0, local, -1)
        lanes = lax.broadcasted_iota(jnp.int32, (rows, slots), 1)
        return jnp.where(lanes == local, 1.0, 0.0).astype(BF16)

    @pl.when(step == 0)
    def _():
        owned_ref[...] = dot(matched(), got_ref[:, :width], ((0,), (0,))).astype(BF16)

    per_step = kv_ref.shape[0] // block
    span = block * cache_len
    same_slot = (
        lax.broadcasted_iota(jnp.int32, (pair * block, span), 0) % block
        == lax.broadcasted_iota(jnp.int32, (pair * block, span), 1) // cache_len
    )
    head_of_row = lax.broadcasted_iota(jnp.int32, (pair * block, pair * HD), 0) // block
    head_of_lane = lax.broadcasted_iota(jnp.int32, (pair * block, pair * HD), 1) // HD
    same_head = head_of_row == head_of_lane
    lanes = lax.broadcasted_iota(jnp.int32, (block, LANES), 1)
    for i in range(per_step):
        start = pl.multiple_of((step * per_step + i) * block, block)
        bias = bias_ref[pl.ds(step * per_step + i, 1), :]
        sums = jnp.where(lanes == 3 * heads, 1.0, 0.0)
        for j in range(heads // pair):
            cols = slice(j * pair * HD, (j + 1) * pair * HD)
            query = owned_ref[pl.ds(start, block), cols]
            spread = jnp.where(same_head, jnp.concatenate([query] * pair, axis=0), 0).astype(BF16)
            keys = kv_ref[i * block:(i + 1) * block, 0, :, cols].reshape(span, pair * HD)
            values = kv_ref[i * block:(i + 1) * block, 1, :, cols].reshape(span, pair * HD)
            scores = dot(spread, keys, ((1,), (1,))) * scale
            scores = jnp.where(same_slot, scores + bias, -jnp.inf)
            top = jnp.max(scores, axis=1, keepdims=True)
            raw = jnp.exp(scores - top)
            total = jnp.sum(raw, axis=1, keepdims=True)
            mixed = dot(raw.astype(BF16), values) / total
            log_sum = top + jnp.log(total)
            for k in range(pair):
                h = j * pair + k
                mixed_ref[pl.ds(start, block), h * HD:(h + 1) * HD] = mixed[
                    k * block:(k + 1) * block, k * HD:(k + 1) * HD
                ].astype(BF16)
                part = log_sum[k * block:(k + 1) * block, :]
                high = part.astype(BF16).astype(F32)
                middle = (part - high).astype(BF16).astype(F32)
                low = (part - high) - middle
                sums = jnp.where(lanes == h, high, sums)
                sums = jnp.where(lanes == heads + h, middle, sums)
                sums = jnp.where(lanes == 2 * heads + h, low, sums)
        mixed_ref[pl.ds(start, block), width:] = sums.astype(BF16)

    @pl.when(step == pl.num_programs(0) - 1)
    def _():
        back_ref[...] = dot(matched(), mixed_ref[...]).astype(BF16)


def attend(got, kv_cache, lengths, block, per_step):
    rows, padded = got.shape
    width = padded - LANES
    heads = width // HD
    slots, _, cache_len, _ = kv_cache.shape
    pair = 2 if heads % 2 == 0 else 1
    bias = jnp.where(
        jnp.arange(cache_len, dtype=jnp.int32)[None, :] < lengths[:, None], F32(0), F32(-1e30)
    ).reshape(slots // block, block * cache_len)
    step_slots = block * per_step
    return pl.pallas_call(
        functools.partial(attend_kernel, heads, block, pair),
        grid=(slots // step_slots,),
        out_shape=jax.ShapeDtypeStruct((rows, padded), BF16),
        in_specs=[
            pl.BlockSpec((rows, padded), lambda i: (0, 0)),
            pl.BlockSpec(bias.shape, lambda i: (0, 0)),
            pl.BlockSpec((step_slots, 2, cache_len, width), lambda i: (i, 0, 0, 0)),
        ],
        out_specs=pl.BlockSpec((rows, padded), lambda i: (0, 0)),
        scratch_shapes=[pltpu.VMEM((slots, width), BF16), pltpu.VMEM((slots, padded), BF16)],
        compiler_params=pltpu.CompilerParams(dimension_semantics=("arbitrary",)),
        cost_estimate=cost(4 * rows * slots * padded, 2 * kv_cache.size),
        name="attend",
    )(got, bias, kv_cache)


def merge_kernel(heads, back_ref, placing_ref, fresh_ref, out_ref):
    width = heads * HD
    scale = HD ** (-0.5)
    rows = dot(placing_ref[...], back_ref[...], ((0,), (0,)))
    tail = rows[:, width:]
    valid = tail[:, 3 * heads:3 * heads + 1] > 0
    for h in range(heads):
        cols = slice(h * HD, (h + 1) * HD)
        query, key, value = (fresh_ref[k, :, cols].astype(F32) for k in range(3))
        own = jnp.sum(query * key, axis=1, keepdims=True) * scale
        log_sum = (
            tail[:, h:h + 1] + tail[:, heads + h:heads + h + 1]
        ) + tail[:, 2 * heads + h:2 * heads + h + 1]
        top = jnp.maximum(own, log_sum)
        cached_raw = jnp.exp(log_sum - top)
        own_raw = jnp.exp(own - top)
        total = cached_raw + own_raw
        mixed = (cached_raw / total) * rows[:, cols] + (own_raw / total) * value
        out_ref[:, cols] = jnp.where(valid, mixed, 0.0).astype(BF16)


def merge(back, placing, fresh):
    streams, width = fresh.shape[1:]
    return pl.pallas_call(
        functools.partial(merge_kernel, width // HD),
        out_shape=jax.ShapeDtypeStruct((streams, width), BF16),
        in_specs=[vmem()] * 3,
        out_specs=vmem(),
        cost_estimate=cost(2 * streams * back.size, 2 * (back.size + fresh.size)),
        name="merge",
    )(back, placing, fresh)


def own_kernel(where_ref, rows_ref, w_ref, residual_ref, out_ref):
    out_ref[...] = residual_ref[...].astype(F32) + dot(rows_ref[...], w_ref[...])


def project_own(rows, w_out, residual, place, tile):
    streams, width = rows.shape
    out_cols = residual.shape[1]
    tiles = out_cols // tile
    return pl.pallas_call(
        own_kernel,
        grid_spec=pltpu.PrefetchScalarGridSpec(
            num_scalar_prefetch=1,
            grid=(tiles,),
            in_specs=[
                pl.BlockSpec((streams, width), lambda i, p: (0, 0)),
                pl.BlockSpec((width, tile), lambda i, p: (0, p[0] * tiles + i)),
                pl.BlockSpec((streams, tile), lambda i, p: (0, i)),
            ],
            out_specs=pl.BlockSpec((streams, tile), lambda i, p: (0, i)),
        ),
        out_shape=jax.ShapeDtypeStruct((streams, out_cols), F32),
        cost_estimate=cost(2 * rows.size * out_cols, 2 * width * out_cols),
        name="project_own",
    )(place, rows, w_out, residual)


def rest_kernel(count, where_ref, sum_ref, *refs):
    out_ref = refs[-1]
    half = refs[1].shape[0]
    mine = pl.multiple_of(where_ref[1] * half, half)
    other = pl.multiple_of((1 - where_ref[1]) * half, half)
    total = sum_ref[...]
    for k in range(count):
        rows_ref, first_ref, second_ref = refs[3 * k:3 * k + 3]
        total += dot(rows_ref[:, pl.ds(mine, half)], first_ref[...])
        total += dot(rows_ref[:, pl.ds(other, half)], second_ref[...])
    out_ref[...] = total.astype(out_ref.dtype)


def project_rest(partial, pieces, place, tile):
    streams, out_cols = partial.shape
    specs, operands = [], []
    for rows, first, second in pieces:
        specs += [
            pl.BlockSpec(rows.shape, lambda i, p: (0, 0)),
            pl.BlockSpec((first.shape[0], tile), lambda i, p: (0, i)),
            pl.BlockSpec((second.shape[0], tile), lambda i, p: (0, i)),
        ]
        operands += [rows, first, second]
    return pl.pallas_call(
        functools.partial(rest_kernel, len(pieces)),
        grid_spec=pltpu.PrefetchScalarGridSpec(
            num_scalar_prefetch=1,
            grid=(out_cols // tile,),
            in_specs=[pl.BlockSpec((streams, tile), lambda i, p: (0, i))] + specs,
            out_specs=pl.BlockSpec((streams, tile), lambda i, p: (0, i)),
        ),
        out_shape=jax.ShapeDtypeStruct((streams, out_cols), BF16),
        cost_estimate=cost(2 * streams * out_cols * 1024, 4 * streams * out_cols),
        name="project_rest",
    )(place, partial, *operands)


def body(residual, fresh_qkv, active, home_slot, kv_cache, lengths, w_out):
    groups = lax.axis_size("dp")
    parts = lax.axis_size("tensor")
    group_here = lax.axis_index("dp")
    part_here = lax.axis_index("tensor")
    streams = home_slot.shape[0]
    width = fresh_qkv.shape[2]
    capacity = max(2, streams // groups)
    out_cols = residual.shape[1]
    half = width // 2
    core = group_here % 2
    place = jnp.stack([part_here, core]).astype(jnp.int32)

    swap = [(i, i ^ 1) for i in range(groups)]
    weights = []
    for k in range(1, parts):
        ring = [(i, (i + k) % parts) for i in range(parts)]
        to = (part_here + k) % parts
        block = lax.dynamic_slice(w_out, (core * half, to * out_cols), (half, out_cols))
        first = lax.ppermute(block, "tensor", ring)
        second = lax.ppermute(first, "dp", swap)
        weights.append((ring, first, second))

    fresh = jnp.transpose(fresh_qkv, (1, 0, 2))
    send, placing = route(home_slot, active, fresh[0], capacity, groups)
    padded = width + LANES

    def exchange(rows):
        rows = rows.reshape(groups, capacity, padded)
        rows = lax.all_to_all(rows, "dp", split_axis=0, concat_axis=0, tiled=True)
        return rows.reshape(groups * capacity, padded)

    back = attend(exchange(send), kv_cache, lengths, 16, 4)
    rows = merge(exchange(back), placing, fresh)
    pieces = [
        (lax.ppermute(rows, "tensor", ring), first, second) for ring, first, second in weights
    ]
    partial = project_own(rows, w_out, residual, place, min(512, out_cols))
    return project_rest(partial, pieces, place, min(512, out_cols))


def solution(mesh):
    placed = (
        P("dp", "tensor"),
        P("dp", None, "tensor"),
        P("dp"),
        P("dp"),
        P("dp", None, None, "tensor"),
        P("dp"),
        P("tensor", None),
    )
    return jax.shard_map(
        body, mesh=mesh, in_specs=placed, out_specs=P("dp", "tensor"), check_vma=False
    )
```

```python
import functools

import jax
import jax.numpy as jnp
from jax import lax
from jax.experimental import pallas as pl
from jax.experimental.pallas import tpu as pltpu
from jax.sharding import PartitionSpec as P


HD = 128
LANES = 128
ID_BASE = 128
F32 = jnp.float32
BF16 = jnp.bfloat16


def vmem():
    return pl.BlockSpec(memory_space=pltpu.VMEM)


def on_chip(*arrays):
    return [pltpu.with_memory_space_constraint(a, pltpu.VMEM) for a in arrays]


def off_chip(*arrays):
    return [pltpu.with_memory_space_constraint(a, pltpu.HBM) for a in arrays]


def limit(mebibytes):
    return pltpu.CompilerParams(vmem_limit_bytes=mebibytes << 20)


def dot(a, b, dims=((1,), (0,))):
    return lax.dot_general(a, b, (dims, ((), ())), preferred_element_type=F32)


def cost(flops, bytes_accessed):
    return pl.CostEstimate(flops=flops, bytes_accessed=bytes_accessed, transcendentals=0)


def place_rows(streams, here, home, active):
    rows = home.shape[1]
    is_active = active > 0
    owner = home // streams
    code_row = jnp.where(is_active, owner, -1).astype(F32)
    code_col = jnp.transpose(jnp.broadcast_to(code_row, (rows, rows)))
    before = lax.broadcasted_iota(jnp.int32, (rows, rows), 0) < lax.broadcasted_iota(
        jnp.int32, (rows, rows), 1
    )
    rank = jnp.sum(
        jnp.where((code_col == code_row) & before, 1.0, 0.0), axis=0, keepdims=True
    ).astype(jnp.int32)
    return owner, owner ^ here, rank, is_active


def one_hot(rows, target):
    hits = lax.broadcasted_iota(jnp.int32, (rows, target.shape[1]), 0) == target
    return jnp.where(hits, 1.0, 0.0).astype(BF16)


def route_kernel(
    capacity, parts, chips, cuts, place_ref, home_ref, active_ref, query_ref, w_ref, *rest
):
    count = len(cuts) * (parts - 1)
    send_refs, block_refs, sems = rest[:-count - 1], rest[-count - 1:-1], rest[-1]
    rows = sum(send_ref.shape[0] for send_ref in send_refs)
    streams, width = query_ref.shape
    copies = []
    for i, block_ref in enumerate(block_refs):
        to = lax.rem(place_ref[0] + i // len(cuts) + 1, parts)
        size, cols = block_ref.shape
        at = cuts[i % len(cuts)][0](place_ref[1], place_ref[3])
        copies.append(
            pltpu.make_async_copy(
                w_ref.at[
                    pl.ds(pl.multiple_of(at, size), size),
                    pl.ds(pl.multiple_of(to * cols, cols), cols),
                ],
                block_ref,
                sems.at[i],
            )
        )
    for copy in copies:
        copy.start()
    home = home_ref[...]
    owner, relative, rank, is_active = place_rows(streams, place_ref[2], home, active_ref[...])
    if chips:
        relative = (relative & 1) * chips + relative // 2
    placing = one_hot(rows, jnp.where(is_active, relative * capacity + rank, -1))
    queries = dot(placing, query_ref[...]).astype(BF16)
    local = home - owner * streams
    kind = lax.broadcasted_iota(jnp.int32, (LANES, streams), 0)
    ids = jnp.where(
        kind == 0, local // ID_BASE, jnp.where(kind == 1, local % ID_BASE, jnp.where(kind == 2, 1, 0))
    )
    ids = dot(placing, ids.astype(F32).astype(BF16), ((1,), (1,))).astype(BF16)
    size = send_refs[0].shape[0]
    for i, send_ref in enumerate(send_refs):
        send_ref[:, :width] = queries[i * size:(i + 1) * size]
        send_ref[:, width:] = ids[i * size:(i + 1) * size]
    for copy in copies:
        copy.wait()


def route(home, active, fresh, w_out, place, capacity, groups, parts, chips, cuts):
    _, streams, width = fresh.shape
    rows = groups * capacity
    blocks = [pltpu.VMEM((size, w_out.shape[1] // parts), BF16) for _, size in cuts] * (parts - 1)
    halves = 2 if chips else 1
    sends = [pltpu.VMEM((rows // halves, width + LANES), BF16)] * halves
    out = pl.pallas_call(
        functools.partial(route_kernel, capacity, parts, chips, cuts),
        grid_spec=pltpu.PrefetchScalarGridSpec(
            num_scalar_prefetch=1,
            grid=(1,),
            in_specs=[
                pl.BlockSpec((1, streams), lambda i, p: (0, 0)),
                pl.BlockSpec((1, streams), lambda i, p: (0, 0)),
                pl.BlockSpec((None, streams, width), lambda i, p: (0, 0, 0)),
                pl.BlockSpec(memory_space=pl.ANY),
            ],
            out_specs=[vmem()] * (halves + len(blocks)),
            scratch_shapes=[pltpu.SemaphoreType.DMA((len(blocks),))],
        ),
        out_shape=sends + blocks,
        cost_estimate=cost(2 * rows * streams * (width + LANES), 4 * streams * width),
        compiler_params=limit(16),
        name="route",
    )(place, *off_chip(home, active, fresh, w_out))
    return out[:halves], out[halves:]


def rows_kernel(
    capacity,
    place_ref,
    home_ref,
    active_ref,
    lengths_ref,
    fresh_hbm,
    cache_hbm,
    placing_ref,
    value_ref,
    own_ref,
    bias_ref,
    cache_ref,
    fresh_ref,
    sems,
):
    pieces = sems.shape[0] - 1
    size = cache_ref.shape[0] // pieces
    first = pltpu.make_async_copy(fresh_hbm, fresh_ref, sems.at[pieces])
    first.start()
    copies = [
        pltpu.make_async_copy(
            cache_hbm.at[pl.ds(i * size, size)], cache_ref.at[pl.ds(i * size, size)], sems.at[i]
        )
        for i in range(pieces)
    ]
    for copy in copies:
        copy.start()
    rows, width = value_ref.shape
    streams = home_ref.shape[1]
    heads = width // HD
    _, relative, rank, is_active = place_rows(streams, place_ref[2], home_ref[...], active_ref[...])
    placing = one_hot(rows, jnp.where(is_active, relative * capacity + rank, -1))
    placing_ref[...] = placing
    first.wait()
    value_ref[...] = dot(placing, fresh_ref[2]).astype(BF16)
    product = dot(placing, fresh_ref[0]) * dot(placing, fresh_ref[1])
    lanes = lax.broadcasted_iota(jnp.int32, own_ref.shape, 1)
    own = jnp.zeros(own_ref.shape, F32)
    for h in range(heads):
        score = jnp.sum(product[:, h * HD:(h + 1) * HD], axis=1, keepdims=True)
        own = jnp.where(lanes == h, score * HD ** (-0.5), own)
    own_ref[...] = own
    blocks, span = bias_ref.shape
    slots = lengths_ref.shape[1]
    block = slots // blocks
    cache_len = span // block
    slot = lax.broadcasted_iota(jnp.int32, (blocks, slots), 1)
    in_block = slot // block == lax.broadcasted_iota(jnp.int32, (blocks, slots), 0)
    length = jnp.where(in_block, lengths_ref[...], 0).astype(F32).astype(BF16)
    slot = lax.broadcasted_iota(jnp.int32, (slots, span), 0)
    spread = slot % block == lax.broadcasted_iota(jnp.int32, (slots, span), 1) // cache_len
    length = dot(length, jnp.where(spread, 1.0, 0.0).astype(BF16))
    position = lax.broadcasted_iota(jnp.int32, bias_ref.shape, 1) % cache_len
    bias_ref[...] = jnp.where(position.astype(F32) < length, 0.0, -1e30)
    for copy in copies:
        copy.wait()


def own_rows(home, active, lengths, fresh, cache, place, capacity, groups, block, pieces=4):
    _, streams, width = fresh.shape
    rows = groups * capacity
    slots, cache_len = cache.shape[0], cache.shape[2]
    whole = pl.BlockSpec(memory_space=pl.ANY)
    return pl.pallas_call(
        functools.partial(rows_kernel, capacity),
        grid_spec=pltpu.PrefetchScalarGridSpec(
            num_scalar_prefetch=1,
            grid=(1,),
            in_specs=[
                pl.BlockSpec((1, streams), lambda i, p: (0, 0)),
                pl.BlockSpec((1, streams), lambda i, p: (0, 0)),
                pl.BlockSpec((1, slots), lambda i, p: (0, 0)),
                whole,
                whole,
            ],
            out_specs=[vmem()] * 5,
            scratch_shapes=[
                pltpu.VMEM(fresh.shape, BF16),
                pltpu.SemaphoreType.DMA((pieces + 1,)),
            ],
        ),
        out_shape=[
            pltpu.VMEM((rows, streams), BF16),
            pltpu.VMEM((rows, width), BF16),
            pltpu.VMEM((rows, LANES), F32),
            pltpu.VMEM((slots // block, block * cache_len), F32),
            pltpu.VMEM((slots // 2, *cache.shape[1:]), BF16),
        ],
        cost_estimate=cost(1 << 31, 2 * cache.size),
        compiler_params=limit(16),
        name="own_rows",
    )(place, *off_chip(home, active, lengths, fresh, cache))


def attend_kernel(heads, block, pair, count, per_step, *refs):
    part_refs, (bias_ref, early_ref, late_hbm), refs = refs[:count], refs[count:count + 3], refs[count + 3:]
    out_refs, (owned_ref, mixed_ref, got_ref, late_ref, sems) = refs[:-5], refs[-5:]
    rows, _ = got_ref.shape
    slots = owned_ref.shape[0]
    early = early_ref.shape[0]
    cache_len = early_ref.shape[2]
    width = heads * HD
    scale = HD ** (-0.5)
    pieces = sems.shape[0]
    size = late_ref.shape[0] // pieces
    copies = [
        pltpu.make_async_copy(
            late_hbm.at[pl.ds(early + i * size, size)], late_ref.at[pl.ds(i * size, size)], sems.at[i]
        )
        for i in range(pieces)
    ]
    for copy in copies:
        copy.start()

    at = 0
    for part_ref in part_refs:
        got_ref[at:at + part_ref.shape[0]] = part_ref[...]
        at += part_ref.shape[0]
    tail = got_ref[:, width:].astype(F32)
    local = (tail[:, 0:1] * ID_BASE + tail[:, 1:2]).astype(jnp.int32)
    local = jnp.where(tail[:, 2:3] > 0, local, -1)
    hits = lax.broadcasted_iota(jnp.int32, (rows, slots), 1) == local
    matched = jnp.where(hits, 1.0, 0.0).astype(BF16)
    owned_ref[...] = dot(matched, got_ref[:, :width], ((0,), (0,))).astype(BF16)

    span = block * cache_len
    other_slot = jnp.where(
        lax.broadcasted_iota(jnp.int32, (block, span), 0)
        == lax.broadcasted_iota(jnp.int32, (block, span), 1) // cache_len,
        0.0,
        -1e30,
    )
    head_of_row = lax.broadcasted_iota(jnp.int32, (pair * block, pair * HD), 0) // block
    head_of_lane = lax.broadcasted_iota(jnp.int32, (pair * block, pair * HD), 1) // HD
    same_head = head_of_row == head_of_lane
    lanes = lax.broadcasted_iota(jnp.int32, (block, LANES), 1)
    pairs = [slice(j * pair * HD, (j + 1) * pair * HD) for j in range(heads // pair)]

    def cache(start, which, cols):
        ref, at = (early_ref, start) if start < early else (late_ref, start - early)
        return ref[at:at + block, which, :, cols].reshape(span, pair * HD)

    waited = 0
    for first in range(0, slots, block * per_step):
        starts = range(first, first + block * per_step, block)
        while waited < pieces and early + waited * size < starts[-1] + block:
            copies[waited].wait()
            waited += 1
        scores = []
        for start in starts:
            queries = owned_ref[start:start + block, :]
            parts = []
            for cols in pairs:
                query = queries[:, cols]
                spread = jnp.where(same_head, jnp.concatenate([query] * pair, axis=0), 0)
                parts.append(dot(spread.astype(BF16), cache(start, 0, cols), ((1,), (1,))))
            scores.append(jnp.concatenate(parts, axis=0))
        raws, sums, inverses = [], [], []
        for i, start in enumerate(starts):
            hide = other_slot + bias_ref[start // block:start // block + 1, :]
            masked = scores[i] * scale + jnp.concatenate([hide] * heads, axis=0)
            top = jnp.max(masked, axis=1, keepdims=True)
            raw = jnp.exp(masked - top)
            total = jnp.sum(raw, axis=1, keepdims=True)
            raws.append(raw.astype(BF16))
            sums.append(top + jnp.log(total))
            inverses.append(1.0 / total)
        for i, start in enumerate(starts):
            for j, cols in enumerate(pairs):
                tall_rows = slice(j * pair * block, (j + 1) * pair * block)
                mixed = dot(raws[i][tall_rows], cache(start, 1, cols))
                for k in range(pair):
                    h = j * pair + k
                    mixed_ref[start:start + block, h * HD:(h + 1) * HD] = (
                        mixed[k * block:(k + 1) * block, k * HD:(k + 1) * HD]
                        * inverses[i][h * block:(h + 1) * block]
                    ).astype(BF16)
            high = sums[i].astype(BF16).astype(F32)
            middle = (sums[i] - high).astype(BF16).astype(F32)
            low = (sums[i] - high) - middle
            packed = jnp.where(lanes == 3 * heads, 1.0, 0.0)
            for h in range(heads):
                part = slice(h * block, (h + 1) * block)
                packed = jnp.where(lanes == h, high[part], packed)
                packed = jnp.where(lanes == heads + h, middle[part], packed)
                packed = jnp.where(lanes == 2 * heads + h, low[part], packed)
            mixed_ref[start:start + block, width:] = packed.astype(BF16)

    back = dot(matched, mixed_ref[...]).astype(BF16)
    if len(out_refs) == 1:
        out_refs[0][...] = back
        return
    chips, size, _ = out_refs[0].shape
    for k in range(chips):
        for i, out_ref in enumerate(out_refs):
            at = (2 * k + i) * size
            out_ref[k] = back[at:at + size]


def attend(got, early, kv_cache, bias, block, per_step, capacity, chips, pieces=4):
    rows, padded = sum(part.shape[0] for part in got), got[0].shape[1]
    width = padded - LANES
    heads = width // HD
    slots = kv_cache.shape[0]
    late = slots - early.shape[0]
    pair = 2 if heads % 2 == 0 else 1
    if chips:
        outs = [pltpu.VMEM((chips, capacity, padded), BF16)] * 2
    else:
        outs = [pltpu.VMEM((rows, padded), BF16)]
    return pl.pallas_call(
        functools.partial(attend_kernel, heads, block, pair, len(got), per_step),
        in_specs=[vmem()] * (2 + len(got)) + [pl.BlockSpec(memory_space=pl.ANY)],
        out_specs=[vmem()] * len(outs),
        scratch_shapes=[
            pltpu.VMEM((slots, width), BF16),
            pltpu.VMEM((slots, padded), BF16),
            pltpu.VMEM((rows, padded), BF16),
            pltpu.VMEM((late, *kv_cache.shape[1:]), BF16),
            pltpu.SemaphoreType.DMA((pieces,)),
        ],
        out_shape=outs,
        compiler_params=limit(28),
        cost_estimate=cost(4 * rows * slots * padded, 2 * kv_cache.size),
        name="attend",
    )(*on_chip(*got, bias, early), *off_chip(kv_cache))


def pack_kernel(keep_ref, got_ref, *out_refs):
    capacity = keep_ref.shape[1]
    for k, out_ref in enumerate(out_refs):
        out_ref[:capacity] = keep_ref[k]
        out_ref[capacity:] = got_ref[k]


def pack(keep, got):
    chips, capacity, padded = keep.shape
    return pl.pallas_call(
        pack_kernel,
        in_specs=[vmem()] * 2,
        out_specs=[vmem()] * chips,
        out_shape=[pltpu.VMEM((2 * capacity, padded), BF16)] * chips,
        compiler_params=limit(16),
        cost_estimate=cost(1 << 20, 8 * keep.size),
        name="pack",
    )(*on_chip(keep, got))


def merge_kernel(start, count, heads, value_ref, own_ref, *refs):
    back_refs, out_ref = refs[:count], refs[count]
    width = heads * HD
    at = start
    done = 0
    for back_ref in back_refs:
        size = back_ref.shape[0]
        rows = back_ref[...].astype(F32)
        tail = rows[:, width:]
        here = slice(at, at + size)
        own = own_ref[here, :heads]
        log_sum = (tail[:, :heads] + tail[:, heads:2 * heads]) + tail[:, 2 * heads:3 * heads]
        top = jnp.maximum(own, log_sum)
        cached_raw = jnp.exp(log_sum - top)
        own_raw = jnp.exp(own - top)
        total = cached_raw + own_raw
        cached_weight, own_weight = cached_raw / total, own_raw / total
        for h in range(heads):
            cols = slice(h * HD, (h + 1) * HD)
            mixed = cached_weight[:, h:h + 1] * rows[:, cols] + own_weight[:, h:h + 1] * value_ref[
                here, cols
            ].astype(F32)
            out_ref[done:done + size, cols] = mixed.astype(BF16)
        at += size
        done += size


def merge(backs, value, own, start):
    width = value.shape[1]
    size = sum(back.shape[0] for back in backs)
    return pl.pallas_call(
        functools.partial(merge_kernel, start, len(backs), width // HD),
        out_shape=pltpu.VMEM((size, width), BF16),
        in_specs=[vmem()] * (2 + len(backs)),
        out_specs=vmem(),
        cost_estimate=cost(1 << 24, 4 * size * width),
        compiler_params=limit(16),
        name="merge",
    )(*on_chip(value, own, *backs))


def in_stream_order(placing_ref, row_refs):
    total, at = None, 0
    for row_ref in row_refs:
        size = row_ref.shape[0]
        part = dot(placing_ref[at:at + size, :], row_ref[...], ((0,), (0,)))
        total = part if total is None else total + part
        at += size
    return total.astype(BF16)


def own_kernel(count, where_ref, placing_ref, *refs):
    row_refs, (w_ref, residual_ref, out_ref, rows_ref) = refs[:count], refs[count:]
    tile = w_ref.shape[1]

    @pl.when(pl.program_id(0) == 0)
    def _():
        rows_ref[...] = in_stream_order(placing_ref, row_refs)

    cols = pl.ds(pl.multiple_of(pl.program_id(0) * tile, tile), tile)
    out_ref[:, cols] = residual_ref[...].astype(F32) + dot(rows_ref[...], w_ref[...])


def project_own(placing, rows, w_out, residual, place, tile):
    streams, out_cols = residual.shape
    width = w_out.shape[0]
    tiles = out_cols // tile
    return pl.pallas_call(
        functools.partial(own_kernel, len(rows)),
        grid_spec=pltpu.PrefetchScalarGridSpec(
            num_scalar_prefetch=1,
            grid=(tiles,),
            in_specs=[vmem()] * (1 + len(rows))
            + [
                pl.BlockSpec((width, tile), lambda i, p: (0, p[0] * tiles + i)),
                pl.BlockSpec((streams, tile), lambda i, p: (0, i)),
            ],
            out_specs=vmem(),
            scratch_shapes=[pltpu.VMEM((streams, width), BF16)],
        ),
        out_shape=pltpu.VMEM((streams, out_cols), F32),
        cost_estimate=cost(2 * streams * width * out_cols, 2 * width * out_cols),
        compiler_params=limit(16),
        name="project_own",
    )(place, *on_chip(placing, *rows), *off_chip(w_out, residual))


def rest_kernel(rings, count, offsets, where_ref, placing_ref, sum_ref, *refs):
    out_ref, rows_ref = refs[-2:]
    tile = out_ref.shape[1]
    cols = pl.ds(pl.multiple_of(pl.program_id(0) * tile, tile), tile)
    each = len(refs[:-2]) // rings
    pieces = [refs[k * each:(k + 1) * each] for k in range(rings)]

    @pl.when(pl.program_id(0) == 0)
    def _():
        for k, piece in enumerate(pieces):
            rows_ref[k] = in_stream_order(placing_ref, piece[:count])

    total = sum_ref[:, cols]
    for k, piece in enumerate(pieces):
        for offset, w_ref in zip(offsets, piece[count:]):
            size = w_ref.shape[0]
            at = pl.multiple_of(offset(where_ref[1], where_ref[3]), size)
            total += dot(rows_ref[k, :, pl.ds(at, size)], w_ref[:, cols])
    out_ref[...] = total.astype(out_ref.dtype)


def project_rest(placing, partial, pieces, offsets, place, tile, width):
    streams, out_cols = partial.shape
    rings, count = len(pieces), len(pieces[0]) - len(offsets)
    operands = [array for piece in pieces for array in piece]
    return pl.pallas_call(
        functools.partial(rest_kernel, rings, count, offsets),
        grid_spec=pltpu.PrefetchScalarGridSpec(
            num_scalar_prefetch=1,
            grid=(out_cols // tile,),
            in_specs=[vmem()] * (2 + len(operands)),
            out_specs=pl.BlockSpec((streams, tile), lambda i, p: (0, i)),
            scratch_shapes=[pltpu.VMEM((rings, streams, width), BF16)],
        ),
        out_shape=jax.ShapeDtypeStruct((streams, out_cols), BF16),
        cost_estimate=cost(2 * streams * out_cols * 1024, 4 * streams * out_cols),
        compiler_params=limit(16),
        name="project_rest",
    )(place, *on_chip(placing, partial, *operands))


def block_step(residual, fresh_qkv, active, home_slot, kv_cache, lengths, w_out):
    groups = lax.axis_size("dp")
    parts = lax.axis_size("tensor")
    group_here = lax.axis_index("dp")
    part_here = lax.axis_index("tensor")
    streams = home_slot.shape[0]
    width = fresh_qkv.shape[2]
    capacity = max(2, streams // groups)
    padded = width + LANES
    rows = groups * capacity
    tile = min(512, residual.shape[1])
    chips = groups // 2 if capacity % 16 == 0 else 0
    here = group_here if chips else 0
    place = jnp.stack([part_here, group_here % 2, here, group_here // 2 % 2]).astype(jnp.int32)
    swap = [(i, i ^ 1) for i in range(groups)]
    rings = [[(i, (i + k) % parts) for i in range(parts)] for k in range(1, parts)]
    block = 16

    def exchange(sent):
        if not chips:
            sent = sent[0].reshape(groups, capacity, padded)
            sent = lax.all_to_all(sent, "dp", split_axis=0, concat_axis=0, tiled=True)
            return [sent.reshape(rows, padded)]
        keep, give = (half.reshape(chips, capacity, padded) for half in sent)
        packed = pack(keep, lax.ppermute(give, "dp", swap))
        parts = [packed[0]]
        for k in range(1, chips):
            parts.append(lax.ppermute(packed[k], "dp", [(i, i ^ (2 * k)) for i in range(groups)]))
        return parts

    half, unit = width // 2, width // 8
    across = [(i, i ^ 2) for i in range(groups)]
    split = unit % LANES == 0 and groups % 4 == 0
    if split:
        cuts = [
            (lambda core, side: core * half + side * 3 * unit, unit),
            (lambda core, side: core * half + unit, unit),
            (lambda core, side: core * half + 2 * unit, unit),
        ]
        offsets = [cut[0] for cut in cuts]
        offsets.append(lambda core, side: core * half + (1 - side) * 3 * unit)
    else:
        cuts = [(lambda core, side: core * half, half)]
        offsets = [cuts[0][0]]
    flip = [lambda core, side, at=at: at(1 - core, side) for at in offsets]

    home = home_slot.reshape(1, streams)
    live = active.reshape(1, streams)
    fresh = jnp.transpose(fresh_qkv, (1, 0, 2))
    sent, blocks = route(home, live, fresh, w_out, place, capacity, groups, parts, chips, cuts)
    weights = [
        [lax.ppermute(block, "tensor", ring) for block in blocks[i * len(cuts):(i + 1) * len(cuts)]]
        for i, ring in enumerate(rings)
    ]
    placing, value, own, bias, early = own_rows(
        home, live, lengths.reshape(1, -1), fresh, kv_cache, place, capacity, groups, block
    )
    if split:
        for fetched in weights:
            shared, _ = lax.optimization_barrier((fetched[0], bias))
            fetched.append(lax.ppermute(shared, "dp", across))
    got = exchange(sent)
    chunks = exchange(attend(got, early, kv_cache, bias, block, 4, capacity, chips))
    bounds = [chunks[:chips // 2], chunks[chips // 2:]] if chips else [chunks]
    merged, at = [], 0
    for some in bounds:
        merged.append(merge(some, value, own, at))
        at += sum(chunk.shape[0] for chunk in some)
    pieces = []
    for ring, fetched in zip(rings, weights):
        theirs = []
        for part in merged:
            theirs.append(lax.ppermute(part, "tensor", ring))
        *fetched, _ = lax.optimization_barrier((*fetched, merged[0]))
        swapped = [lax.ppermute(some, "dp", swap) for some in fetched]
        pieces.append((*theirs, *fetched, *swapped))
    partial = project_own(placing, merged, w_out, residual, place, tile)
    return project_rest(placing, partial, pieces, offsets + flip, place, tile, width)


def solution(mesh):
    placed = (
        P("dp", "tensor"),
        P("dp", None, "tensor"),
        P("dp"),
        P("dp"),
        P("dp", None, None, "tensor"),
        P("dp"),
        P("tensor", None),
    )
    return jax.shard_map(
        block_step, mesh=mesh, in_specs=placed, out_specs=P("dp", "tensor"), check_vma=False
    )
```
